32 devices in a mesh: qrow: 8 (over y, x, core), kcol: 4 (over z).
Axes of the slice: x: 2, y: 2, z: 4, core: 2. Of those that a mesh axis runs over, the one named last changes fastest.
Arguments:
- query_states: bfloat16 [32768, 512], P(('qrow', 'kcol')), may hold values from -8 to 8
- key_states: bfloat16 [32768, 512], P(('kcol', 'qrow')), may hold values from -8 to 8
- value_states: bfloat16 [32768, 512], P(('kcol', 'qrow')), may hold values from -6 to 6
- saved_output: bfloat16 [32768, 512], P(('qrow', 'kcol')), may hold values from -0.59765625 to 0.59765625
- output_grad: bfloat16 [32768, 512], P(('qrow', 'kcol')), may hold values from -6 to 6
- normalizer: float32 [32768, 4], P(('qrow', 'kcol')), as said below
- doc_lengths: int32 [8], replicated, may hold values from 1 to 8192, as said below
Outputs:
- query_grad: bfloat16 [32768, 512], P(('qrow', 'kcol'))
- key_grad: bfloat16 [32768, 512], P(('kcol', 'qrow'))
- value_grad: bfloat16 [32768, 512], P(('kcol', 'qrow'))
The draws below stay inside these ranges and needn't reach their ends.
Inputs may be any that keep to these rules, and one draw needn't show every extreme that they name: `doc_lengths`: the 8 lengths sum to 32768; exactly one of them equals 8192, every other one is smaller. normalizer[p, h] is the logarithm of the sum of exp(scores[h, p, t]) over the t that allowed admits, computed in float32 from query_states, key_states and doc_lengths.
All inputs are finite; a program needn't handle non-finite values.
Results may differ from the reference program's by a relative error of at most 0.005.
Values may be sent and summed in bfloat16 or wider, within the bound.
A program may use at most 704 MiB of HBM per device.

```python
import jax
import jax.numpy as jnp
from jax import lax

HEAD_DIM = 128
KV_HEADS = 4
GROUP = 1
TOK = 32768
DOCS = 8
MOST = 8192


def make_queries(key):
    sample = jnp.clip(jax.random.normal(jax.random.fold_in(key, 101), (TOK, KV_HEADS * GROUP * HEAD_DIM), jnp.float32), -4.0, 4.0)
    return sample.astype(jnp.bfloat16)


def make_keys(key):
    sample = jnp.clip(jax.random.normal(jax.random.fold_in(key, 201), (TOK, KV_HEADS * HEAD_DIM), jnp.float32), -4.0, 4.0)
    return sample.astype(jnp.bfloat16)


def make_lengths(key):
    weights = jax.random.randint(jax.random.fold_in(key, 301), (DOCS - 1,), 2, 4).astype(jnp.int32)
    remaining = TOK - MOST - (DOCS - 1)
    others = 1 + remaining * weights // jnp.sum(weights)
    leftover = TOK - MOST - jnp.sum(others)
    others = others + (jnp.arange(DOCS - 1, dtype=jnp.int32) < leftover).astype(jnp.int32)
    longest_at = jax.random.randint(jax.random.fold_in(key, 302), (), 0, DOCS).astype(jnp.int32)
    places = jnp.arange(DOCS, dtype=jnp.int32)
    source = jnp.clip(places - (places > longest_at).astype(jnp.int32), 0, DOCS - 2)
    return jnp.where(places == longest_at, MOST, others[source]).astype(jnp.int32)


def draw_query_states(key, part):
    return make_queries(key)


def draw_key_states(key, part):
    return make_keys(key)


def draw_doc_lengths(key, part):
    return make_lengths(key)


def draw_normalizer(key, part):
    scaling = HEAD_DIM ** (-0.5)
    queries = make_queries(key).astype(jnp.float32).reshape(TOK, KV_HEADS, GROUP, HEAD_DIM).transpose(1, 0, 2, 3)
    keys_all = make_keys(key).astype(jnp.float32).reshape(TOK, KV_HEADS, HEAD_DIM).transpose(1, 0, 2)
    lengths = make_lengths(key)
    positions = jnp.arange(TOK, dtype=jnp.int32)
    doc_ends = jnp.cumsum(lengths)
    documents = jnp.sum((positions[:, None] >= doc_ends[None, :]).astype(jnp.int32), axis=1)
    block_rows = 512 if TOK % 512 == 0 else TOK
    block_count = TOK // block_rows
    window = min(block_rows + MOST, TOK)

    def per_head(operands):
        query_head, key_head = operands

        def per_block(block_index):
            start_row = block_index * block_rows
            key_start = jnp.clip(start_row - MOST, 0, TOK - window).astype(jnp.int32)
            query_rows = lax.dynamic_slice_in_dim(query_head, start_row, block_rows, 0)
            key_rows = lax.dynamic_slice_in_dim(key_head, key_start, window, 0)
            key_pos = lax.dynamic_slice_in_dim(positions, key_start, window, 0)
            key_doc = lax.dynamic_slice_in_dim(documents, key_start, window, 0)
            query_pos = start_row + jnp.arange(block_rows, dtype=jnp.int32)
            query_doc = lax.dynamic_slice_in_dim(documents, start_row, block_rows, 0)
            allowed = (key_pos[None, :] <= query_pos[:, None]) & (key_doc[None, :] == query_doc[:, None])
            scores = jnp.einsum('qgd,kd->qgk', query_rows, key_rows) * scaling
            masked = jnp.where(allowed[:, None, :], scores, -1e+30)
            highest = jnp.max(masked, axis=2, keepdims=True)
            totals = jnp.sum(jnp.where(allowed[:, None, :], jnp.exp(masked - highest), 0.0), axis=2)
            return highest[:, :, 0] + jnp.log(totals)
        return lax.map(per_block, jnp.arange(block_count, dtype=jnp.int32)).reshape(TOK, GROUP)
    result = lax.map(per_head, (queries, keys_all))
    return result.transpose(1, 0, 2).reshape(TOK, KV_HEADS * GROUP).astype(jnp.float32)


def level_of(stream_key, shape, split, smallest, largest):
    def one(position, parts):
        draws = jax.random.uniform(jax.random.fold_in(jax.random.fold_in(stream_key, 6), position), (parts,), jnp.float32, smallest / len(split), largest / len(split))
        return jnp.repeat(jnp.exp(draws), shape[position] // parts).reshape((-1,) + (1,) * (len(shape) - position - 1))

    factor_of = one(*split[0])
    for cut in split[1:]:
        factor_of = factor_of * one(*cut)
    return factor_of


def gaussian(key, dims, deviation, most, shards=(), kind=jnp.bfloat16):
    loudness = level_of(key, dims, shards, -0.22, 0.18) if shards else 1.0
    array = jax.random.normal(key, dims, jnp.float32) * deviation * loudness
    return jnp.minimum(jnp.maximum(array, -most), most).astype(kind)


def setup_inputs(seed: int = 0) -> dict:
    arg_keys = jax.random.split(jax.random.key(seed), 8)
    query_states = draw_query_states(jax.random.fold_in(arg_keys[7], 71), 0)
    key_states = draw_key_states(jax.random.fold_in(arg_keys[7], 71), 0)
    value_states = gaussian(arg_keys[2], (TOK, KV_HEADS * HEAD_DIM), 1.0, 6.0, ((0, 32),))
    saved_output = gaussian(arg_keys[3], (TOK, KV_HEADS * GROUP * HEAD_DIM), 0.1, 0.59765625, ((0, 32),))
    output_grad = gaussian(arg_keys[4], (TOK, KV_HEADS * GROUP * HEAD_DIM), 1.0, 6.0, ((0, 32),))
    normalizer = draw_normalizer(jax.random.fold_in(arg_keys[7], 71), 0)
    doc_lengths = draw_doc_lengths(jax.random.fold_in(arg_keys[7], 71), 0)
    return {"query_states": query_states, "key_states": key_states, "value_states": value_states, "saved_output": saved_output, "output_grad": output_grad, "normalizer": normalizer, "doc_lengths": doc_lengths}


def document_ids(doc_lengths, positions):
    doc_ends = jnp.cumsum(doc_lengths)
    return jnp.sum((positions[:, None] >= doc_ends[None, :]).astype(jnp.int32), axis=1)


def reference(query_states, key_states, value_states, saved_output, output_grad, normalizer, doc_lengths):
    scaling = HEAD_DIM ** -0.5
    head_count = KV_HEADS * GROUP
    positions = jnp.arange(TOK, dtype=jnp.int32)
    documents = document_ids(doc_lengths, positions)
    row_delta = jnp.sum((output_grad.astype(jnp.float32) * saved_output.astype(jnp.float32)).reshape(TOK, head_count, HEAD_DIM), axis=2)
    block_rows = 512 if TOK % 512 == 0 else TOK
    block_count = TOK // block_rows
    window = min(block_rows + MOST, TOK)
    query_heads = query_states.astype(jnp.float32).reshape(TOK, KV_HEADS, GROUP, HEAD_DIM).transpose(1, 0, 2, 3)
    grad_heads = output_grad.astype(jnp.float32).reshape(TOK, KV_HEADS, GROUP, HEAD_DIM).transpose(1, 0, 2, 3)
    key_heads = key_states.astype(jnp.float32).reshape(TOK, KV_HEADS, HEAD_DIM).transpose(1, 0, 2)
    value_heads = value_states.astype(jnp.float32).reshape(TOK, KV_HEADS, HEAD_DIM).transpose(1, 0, 2)
    norm_heads = normalizer.reshape(TOK, KV_HEADS, GROUP).transpose(1, 0, 2)
    delta_heads = row_delta.reshape(TOK, KV_HEADS, GROUP).transpose(1, 0, 2)

    def one_head(operands):
        query_all, grad_all, key_all, value_all, norm_all, delta_all = operands

        def one_block(running, block_index):
            key_acc, value_acc = running
            start_row = block_index * block_rows
            key_start = jnp.clip(start_row - MOST, 0, TOK - window).astype(jnp.int32)
            query_rows = lax.dynamic_slice_in_dim(query_all, start_row, block_rows, 0)
            grad_rows = lax.dynamic_slice_in_dim(grad_all, start_row, block_rows, 0)
            norm_rows = lax.dynamic_slice_in_dim(norm_all, start_row, block_rows, 0)
            delta_rows = lax.dynamic_slice_in_dim(delta_all, start_row, block_rows, 0)
            key_rows = lax.dynamic_slice_in_dim(key_all, key_start, window, 0)
            value_rows = lax.dynamic_slice_in_dim(value_all, key_start, window, 0)
            key_pos = lax.dynamic_slice_in_dim(positions, key_start, window, 0)
            key_doc = lax.dynamic_slice_in_dim(documents, key_start, window, 0)
            query_pos = start_row + jnp.arange(block_rows, dtype=jnp.int32)
            query_doc = lax.dynamic_slice_in_dim(documents, start_row, block_rows, 0)
            allowed = (key_pos[None, :] <= query_pos[:, None]) & (key_doc[None, :] == query_doc[:, None])
            scores = jnp.einsum("qgd,kd->gqk", query_rows, key_rows) * scaling
            probability = jnp.where(allowed[None], jnp.exp(scores - norm_rows.T[:, :, None]), 0.0)
            prob_grad = jnp.einsum("qgd,kd->gqk", grad_rows, value_rows)
            score_grad = probability * (prob_grad - delta_rows.T[:, :, None])
            prob_half = lax.optimization_barrier(probability.astype(jnp.bfloat16)).astype(jnp.float32)
            grad_half = lax.optimization_barrier(score_grad.astype(jnp.bfloat16)).astype(jnp.float32)
            value_add = jnp.einsum("gqk,qgd->kd", prob_half, grad_rows)
            key_add = jnp.einsum("gqk,qgd->kd", grad_half, query_rows)
            value_acc = lax.dynamic_update_slice_in_dim(value_acc, lax.dynamic_slice_in_dim(value_acc, key_start, window, 0) + value_add, key_start, 0)
            key_acc = lax.dynamic_update_slice_in_dim(key_acc, lax.dynamic_slice_in_dim(key_acc, key_start, window, 0) + key_add, key_start, 0)
            query_part = jnp.einsum("gqk,kd->qgd", grad_half, key_rows) * scaling
            return (key_acc, value_acc), query_part

        empty_rows = jnp.zeros((TOK, HEAD_DIM), jnp.float32)
        (key_acc, value_acc), query_parts = lax.scan(one_block, (empty_rows, empty_rows), jnp.arange(block_count, dtype=jnp.int32))
        return query_parts.reshape(TOK, GROUP, HEAD_DIM), key_acc * scaling, value_acc

    query_all_grad, key_all_grad, value_all_grad = lax.map(one_head, (query_heads, grad_heads, key_heads, value_heads, norm_heads, delta_heads))
    query_grad = query_all_grad.transpose(1, 0, 2, 3).reshape(TOK, head_count * HEAD_DIM).astype(jnp.bfloat16)
    key_grad = key_all_grad.transpose(1, 0, 2).reshape(TOK, KV_HEADS * HEAD_DIM).astype(jnp.bfloat16)
    value_grad = value_all_grad.transpose(1, 0, 2).reshape(TOK, KV_HEADS * HEAD_DIM).astype(jnp.bfloat16)
    return (query_grad, key_grad, value_grad)
```

```python
import functools
import math

import jax
import jax.numpy as jnp
from jax import lax
from jax.experimental import pallas as pl
from jax.experimental.pallas import tpu as pltpu
from jax.sharding import Mesh, PartitionSpec as P

HEAD_DIM = 128
KV_HEADS = 4
TILE_Q = 512
TILE_K = 256
SCALING = HEAD_DIM ** (-0.5)
LOG2E = math.log2(math.e)

Q_AXES = ("yx", "core", "ko", "head")
K_AXES = ("ko", "head", "yx", "core")


def dot(a, b, dims):
    return lax.dot_general(a, b, (dims, ((), ())), preferred_element_type=jnp.float32)


def attention_kernel(
    piece, groups, docs, ends_ref, where_ref, q_ref, g_ref, nd_ref, k_ref, v_ref,
    dq_ref, dk_ref, dv_ref, dq_acc, dk_acc, dv_acc,
):
    tile_q = nd_ref.shape[2]
    tile_k = dk_acc.shape[0]
    q_tiles = q_ref.shape[0] // tile_q
    k_tiles = k_ref.shape[0] // tile_k
    core = where_ref[0]
    group = where_ref[1]
    run = 2 * piece

    def key_token(i):
        return (i // run) * (groups * run) + group * run + i % run

    def doc_end(position):
        end = jnp.zeros_like(position)
        for d in range(docs - 1, -1, -1):
            end = jnp.where(position < ends_ref[d], ends_ref[d], end)
        return end

    dq_acc[...] = jnp.zeros_like(dq_acc)
    q_local = lax.broadcasted_iota(jnp.int32, (1, tile_q), 1)
    q_base = (q_local // piece) * run + core * piece + q_local % piece

    def key_step(kt, carry):
        k_lo = kt * tile_k
        rows = pl.ds(pl.multiple_of(k_lo, tile_k), tile_k)
        k = k_ref[rows, :]
        v = v_ref[rows, :]
        k_t = k.T
        k_pos = key_token(k_lo + lax.broadcasted_iota(jnp.int32, (tile_k, 1), 0))
        k_end = doc_end(k_pos)
        first = key_token(k_lo) // (2 * tile_q)
        last = (doc_end(key_token(k_lo + tile_k - 1)) - 1) // (2 * tile_q)
        dk_acc[...] = jnp.zeros_like(dk_acc)
        dv_acc[...] = jnp.zeros_like(dv_acc)

        def query_step(qt, carry):
            q_rows = pl.ds(pl.multiple_of(qt * tile_q, tile_q), tile_q)
            q = q_ref[q_rows, :]
            g = g_ref[q_rows, :]
            nd = nd_ref[qt]
            norm = nd[0:1, :]
            delta = nd[1:2, :]
            q_pos = q_base + qt * (2 * tile_q)
            s = dot(k, q, ((1,), (1,)))
            dp = dot(v, g, ((1,), (1,)))
            allowed = (k_pos <= q_pos) & (q_pos < k_end)
            p = jnp.where(allowed, jnp.exp2(s * (SCALING * LOG2E) - norm), 0.0)
            ds = (p * (dp - delta)).astype(jnp.bfloat16)
            dv_acc[...] += dot(p.astype(jnp.bfloat16), g, ((1,), (0,)))
            dk_acc[...] += dot(ds, q, ((1,), (0,)))
            dq_acc[qt] += dot(k_t, ds, ((1,), (0,)))
            return carry

        lax.fori_loop(first, last + 1, query_step, 0)
        dk_ref[rows, :] = (dk_acc[...] * SCALING).astype(jnp.bfloat16)
        dv_ref[rows, :] = dv_acc[...].astype(jnp.bfloat16)
        return carry

    lax.fori_loop(0, k_tiles, key_step, 0)

    def finish(qt, carry):
        q_rows = pl.ds(pl.multiple_of(qt * tile_q, tile_q), tile_q)
        dq_ref[q_rows, :] = (dq_acc[qt] * SCALING).T.astype(jnp.bfloat16)
        return carry

    lax.fori_loop(0, q_tiles, finish, 0)


def local_attention(piece, groups, ends, place, q, g, nd, k, v):
    tile_q = nd.shape[2]
    tile_k = min(TILE_K, k.shape[0])
    whole = pl.BlockSpec(memory_space=pltpu.VMEM)
    scalars = pl.BlockSpec(memory_space=pltpu.SMEM)
    return pl.pallas_call(
        functools.partial(attention_kernel, piece, groups, ends.shape[0]),
        out_shape=(
            jax.ShapeDtypeStruct(q.shape, jnp.bfloat16),
            jax.ShapeDtypeStruct(k.shape, jnp.bfloat16),
            jax.ShapeDtypeStruct(v.shape, jnp.bfloat16),
        ),
        in_specs=[scalars, scalars, whole, whole, whole, whole, whole],
        out_specs=(whole, whole, whole),
        scratch_shapes=[
            pltpu.VMEM((q.shape[0] // tile_q, HEAD_DIM, tile_q), jnp.float32),
            pltpu.VMEM((tile_k, HEAD_DIM), jnp.float32),
            pltpu.VMEM((tile_k, HEAD_DIM), jnp.float32),
        ],
        compiler_params=pltpu.CompilerParams(vmem_limit_bytes=58 * 1024 * 1024),
    )(ends, place, q, g, nd, k, v)


def per_device(sizes, query_states, key_states, value_states, saved_output, output_grad,
               normalizer, doc_lengths):
    yx, core, ko, head = (sizes[a] for a in Q_AXES)
    devices = yx * core * ko * head
    rows = query_states.shape[0]
    piece = rows // (yx * ko * core)
    groups = yx * ko
    row_delta = jnp.sum(
        (output_grad.astype(jnp.float32) * saved_output.astype(jnp.float32)).reshape(
            rows, KV_HEADS, HEAD_DIM
        ),
        axis=2,
    )

    def deal(x, key_side):
        x = x.reshape(yx, ko, core, piece, KV_HEADS, -1)
        order = (1, 4, 0, 2, 3, 5) if key_side else (0, 2, 1, 4, 3, 5)
        x = x.transpose(order).reshape(devices, piece, x.shape[-1])
        return lax.all_to_all(x, K_AXES if key_side else Q_AXES, 0, 0, tiled=True)

    def undeal(x, key_side):
        x = lax.all_to_all(x, K_AXES if key_side else Q_AXES, 0, 0, tiled=True)
        if key_side:
            x = x.reshape(ko, head, yx, core, piece, HEAD_DIM).transpose(2, 0, 3, 4, 1, 5)
        else:
            x = x.reshape(yx, core, ko, head, piece, HEAD_DIM).transpose(0, 2, 1, 4, 3, 5)
        return x.reshape(rows, KV_HEADS * HEAD_DIM)

    nd = jnp.stack([normalizer * LOG2E, row_delta], axis=-1)
    nd = deal(nd, False)
    q = deal(query_states, False)
    g = deal(output_grad, False)
    k = deal(key_states, True)
    v = deal(value_states, True)

    def gather(x, axes):
        x = lax.all_gather(x, axes, axis=0, tiled=False)
        return x.transpose(1, 0, 2, 3).reshape(-1, x.shape[-1])

    nd = gather(nd, ("yx", "ko"))
    q = gather(q, ("yx", "ko"))
    g = gather(g, ("yx", "ko"))
    k = gather(k, ("core",))
    v = gather(v, ("core",))
    tile_q = min(TILE_Q, q.shape[0])
    nd = nd.reshape(-1, tile_q, 2).transpose(0, 2, 1)
    place = jnp.stack(
        [lax.axis_index("core"), lax.axis_index("yx") * ko + lax.axis_index("ko")]
    ).astype(jnp.int32)
    ends = jnp.cumsum(doc_lengths)
    dq, dk, dv = local_attention(piece, groups, ends, place, q, g, nd, k, v)

    def total(x, parts, axes):
        x = x.reshape(devices, parts, piece, HEAD_DIM).transpose(1, 0, 2, 3)
        x = lax.all_to_all(x, axes, 0, 0, tiled=True)
        return jnp.sum(x.astype(jnp.float32), axis=0).astype(jnp.bfloat16)

    dq = undeal(total(dq, groups, ("yx", "ko")), False)
    dk = undeal(total(dk, core, ("core",)), True)
    dv = undeal(total(dv, core, ("core",)), True)
    return dq, dk, dv


def solution(mesh):
    qrow = mesh.shape["qrow"]
    kcol = mesh.shape["kcol"]
    sizes = {"yx": qrow // 2, "core": 2, "ko": kcol // KV_HEADS, "head": KV_HEADS}
    fine = Mesh(mesh.devices.reshape([sizes[a] for a in Q_AXES]), Q_AXES)
    by_query = P(Q_AXES, None)
    by_key = P(K_AXES, None)
    return jax.shard_map(
        functools.partial(per_device, sizes),
        mesh=fine,
        in_specs=(by_query, by_key, by_key, by_query, by_query, by_query, P()),
        out_specs=(by_query, by_key, by_key),
        check_vma=False,
    )
```
